32 devices in a mesh: seq: 4 (over y, core), shard: 2 (over x), replica: 4 (over z).
Axes of the slice: x: 2, y: 2, z: 4, core: 2. Of those that a mesh axis runs over, the one named last changes fastest.
Arguments:
- tokens: bfloat16 [8, 1024, 1536], P(('shard', 'replica'), 'seq'), may hold values from -6 to 6
- in_proj: bfloat16 [1536, 6448], P('shard'), may hold values from -0.15625 to 0.15625
- out_proj: bfloat16 [3072, 1536], P('shard'), may hold values from -0.109375 to 0.109375
- pre_gain: bfloat16 [1536], P('shard'), may hold values from 0.5 to 1.5
- conv_weight: bfloat16 [4, 3328], P(None, 'shard'), may hold values from -3 to 3
- conv_bias: bfloat16 [3328], P('shard'), may hold values from -3 to 3
- dt_bias: bfloat16 [48], P('shard'), may hold values from -6 to -3
- a_log: bfloat16 [48], P('shard'), may hold values from -3 to 1.5
- d_skip: bfloat16 [48], P('shard'), may hold values from 0.5 to 1.5
- norm_gain: bfloat16 [3072], P('shard'), may hold values from 0.5 to 1.5
- cotangent: bfloat16 [8, 1024, 1536], P(('shard', 'replica'), 'seq'), may hold values from -6 to 6
Outputs:
- block_out: float32 [8, 1024, 1536], P(('shard', 'replica'), 'seq')
- grad_tokens: float32 [8, 1024, 1536], P(('shard', 'replica'), 'seq')
- grad_in_proj: float32 [1536, 6448], P('shard')
- grad_out_proj: float32 [3072, 1536], P('shard')
- grad_pre_gain: float32 [1536], P('shard')
- grad_conv_weight: float32 [4, 3328], P(None, 'shard')
- grad_conv_bias: float32 [3328], P('shard')
- grad_dt_bias: float32 [48], P('shard')
- grad_a_log: float32 [48], P('shard')
- grad_d_skip: float32 [48], P('shard')
- grad_norm_gain: float32 [3072], P('shard')
The draws below stay inside these ranges and needn't reach their ends.
All inputs are finite; a program needn't handle non-finite values.
Results may differ from the reference program's by a relative error of at most 0.0059.
Values may be sent and summed in bfloat16 or wider, within the bound.
A program may use at most 320 MiB of HBM per device.

```python
import jax
import jax.numpy as jnp
from jax import lax

D = 1536
H = 48
P_SIZE = 64
NSTATE = 128
CONVK = 4
SPAN = 256
SEQ_DEV = 1
INNER = 3072
XBC = 3328
PROJ = 6448
LENGTH = 1024
SEQS = 8
N_SEQ = 4


def block_levels(own_key, dims, shards, low, top_value):
    factor_of, own = 1.0, jax.random.fold_in(own_key, 6)
    for position, shards_of in shards:
        heights = jnp.exp(jax.random.uniform(jax.random.fold_in(own, position), (shards_of,), jnp.float32, low / len(shards), top_value / len(shards)))
        factor_of = factor_of * jnp.repeat(heights, dims[position] // shards_of).reshape([-1 if axis == position else 1 for axis in range(len(dims))])
    return factor_of


def gaussian(stream_key, extent, width, reach, shards=(), held_as=jnp.bfloat16):
    level = block_levels(stream_key, extent, shards, -0.22, 0.18) if shards else 1.0
    entries = jax.random.normal(stream_key, extent, jnp.float32) * width * level
    return jnp.minimum(jnp.maximum(entries, -reach), reach).astype(held_as)


def setup_inputs(seed: int = 0) -> dict:
    splits = jax.random.split(jax.random.key(seed), 12)
    return {
        "tokens": gaussian(splits[0], (SEQS, LENGTH, D), 1.0, 6.0, ((0, 8), (1, 4))),
        "in_proj": gaussian(splits[1], (D, PROJ), D ** -0.5, 0.15625, ((0, 2),)),
        "out_proj": gaussian(splits[2], (INNER, D), INNER ** -0.5, 0.109375, ((0, 2),)),
        "pre_gain": jnp.clip(1.0 + 0.1 * jax.random.normal(splits[3], (D,), jnp.float32), 0.5, 1.5).astype(jnp.bfloat16),
        "conv_weight": gaussian(splits[4], (CONVK, XBC), CONVK ** -0.5, 3.0, ((1, 2),)),
        "conv_bias": gaussian(splits[5], (XBC,), 0.5, 3.0, ((0, 2),)),
        "dt_bias": jnp.clip(-6.0 + 3.0 * jax.random.uniform(splits[6], (H,), jnp.float32) ** block_levels(splits[6], (H,), ((0, 2),), -0.2, 0.2), -6.0, -3.0).astype(jnp.bfloat16),
        "a_log": jnp.clip(-3.0 + 4.5 * jax.random.uniform(splits[7], (H,), jnp.float32) ** block_levels(splits[7], (H,), ((0, 2),), -0.2, 0.2), -3.0, 1.5).astype(jnp.bfloat16),
        "d_skip": jnp.clip(0.5 + 1.0 * jax.random.uniform(splits[8], (H,), jnp.float32) ** block_levels(splits[8], (H,), ((0, 2),), -0.2, 0.2), 0.5, 1.5).astype(jnp.bfloat16),
        "norm_gain": jnp.clip(1.0 + 0.1 * jax.random.normal(splits[9], (INNER,), jnp.float32), 0.5, 1.5).astype(jnp.bfloat16),
        "cotangent": gaussian(splits[10], (SEQS, LENGTH, D), 1.0, 6.0, ((0, 8), (1, 4))),
    }


epsilon = 1e-05
highest = lax.Precision.HIGHEST

def convolve(extended, conv_weight, conv_bias, seq_length):
    total = conv_bias
    for offset in range(CONVK):
        total = total + conv_weight[offset] * extended[:, offset:offset + seq_length]
    return total

def prepare(projected, halo_rows, conv_weight, conv_bias, dt_bias, a_log):
    seq_count, seq_length = (projected.shape[0], projected.shape[1])
    gate_z = projected[..., :INNER]
    extended = jnp.concatenate([halo_rows, projected[..., INNER:INNER + XBC]], axis=1)
    activated = jax.nn.silu(convolve(extended, conv_weight, conv_bias, seq_length))
    values = activated[..., :INNER].reshape(seq_count, seq_length, H, P_SIZE)
    b_state = activated[..., INNER:INNER + NSTATE]
    c_state = activated[..., INNER + NSTATE:]
    step_size = jax.nn.softplus(projected[..., INNER + XBC:] + dt_bias)
    log_decay = -step_size * jnp.exp(a_log)
    return (values, b_state, c_state, step_size, log_decay, gate_z)

def span_local(values, b_state, c_state, step_size, log_decay):
    seq_length = values.shape[1]
    cumulative = jnp.cumsum(log_decay, axis=1)
    inner_bc = jnp.einsum('stn,sun->stu', c_state, b_state, precision=highest)
    lower = jnp.arange(seq_length)[:, None] >= jnp.arange(seq_length)[None, :]
    differ = cumulative[:, :, None, :] - cumulative[:, None, :, :]
    kernel = jnp.exp(jnp.where(lower[None, :, :, None], differ, -10000.0)) * inner_bc[..., None] * step_size[:, None, :, :]
    y_intra = jnp.einsum('stuh,suhp->sthp', kernel, values, precision=highest)
    decays = jnp.exp(cumulative)
    a_total = decays[:, -1, :]
    tail_weight = jnp.exp(cumulative[:, -1:, :] - cumulative) * step_size
    h_local = jnp.einsum('suh,suhp,sun->shpn', tail_weight, values, b_state, precision=highest)
    return (y_intra, decays, a_total, h_local)

def finish(y_intra, decays, c_state, h_enter, values, gate_z, d_skip, norm_gain):
    seq_count, seq_length = (values.shape[0], values.shape[1])
    y_inter = decays[..., None] * jnp.einsum('stn,shpn->sthp', c_state, h_enter, precision=highest)
    y_core = (y_intra + y_inter + d_skip[:, None] * values).reshape(seq_count, seq_length, INNER)
    gated = y_core * jax.nn.silu(gate_z)
    inverse = lax.rsqrt(lax.optimization_barrier(jnp.mean(gated * gated, axis=-1, keepdims=True)) + epsilon)
    return gated * inverse * norm_gain

def middle(projected, conv_weight, conv_bias, dt_bias, a_log, d_skip, norm_gain):
    seq_count = projected.shape[0]
    halo_rows = jnp.zeros((seq_count, CONVK - 1, XBC), jnp.float32)
    prepared = prepare(projected, halo_rows, conv_weight, conv_bias, dt_bias, a_log)
    pieces = tuple((jnp.moveaxis(piece.reshape((seq_count, N_SEQ, SPAN) + piece.shape[2:]), 1, 0) for piece in prepared))

    def advance(state, piece):
        y_intra, decays, a_total, h_local = span_local(piece[0], piece[1], piece[2], piece[3], piece[4])
        mixed = finish(y_intra, decays, piece[2], state, piece[0], piece[5], d_skip, norm_gain)
        return (a_total[:, :, None, None] * state + h_local, mixed)
    start = jnp.zeros((seq_count, H, P_SIZE, NSTATE), jnp.float32)
    final_state, mixed = lax.scan(advance, start, pieces)
    return jnp.moveaxis(mixed, 0, 1).reshape(seq_count, N_SEQ * SPAN, INNER)

def reference(tokens, in_proj, out_proj, pre_gain, conv_weight, conv_bias, dt_bias, a_log, d_skip, norm_gain, cotangent):
    small_params = tuple((piece.astype(jnp.float32) for piece in (conv_weight, conv_bias, dt_bias, a_log, d_skip, norm_gain)))
    pre_wide = pre_gain.astype(jnp.float32)
    blocks = SEQS // SEQ_DEV
    rows_block = SEQ_DEV * LENGTH
    token_blocks = tokens.reshape(blocks, SEQ_DEV, LENGTH, D)
    cot_blocks = cotangent.reshape(blocks, SEQ_DEV, LENGTH, D)

    def one_block(totals, piece):
        token_block, cot_block = piece
        tokens_wide = token_block.astype(jnp.float32)
        inverse = lax.rsqrt(lax.optimization_barrier(jnp.mean(tokens_wide * tokens_wide, axis=-1, keepdims=True)) + epsilon)
        normed = (tokens_wide * inverse * pre_wide).astype(jnp.bfloat16).reshape(rows_block, D)
        projected = jnp.dot(normed, in_proj, preferred_element_type=jnp.float32).reshape(SEQ_DEV, LENGTH, PROJ)
        mixed, middle_back = jax.vjp(middle, projected, *small_params)
        mixed_low = mixed.astype(jnp.bfloat16).reshape(rows_block, INNER)
        branch = jnp.dot(mixed_low, out_proj, preferred_element_type=jnp.float32)
        block_out = tokens_wide + branch.reshape(SEQ_DEV, LENGTH, D)
        cot_rows = cot_block.reshape(rows_block, D)
        grad_out = jnp.dot(mixed_low.T, cot_rows, preferred_element_type=jnp.float32)
        d_mixed = jnp.dot(cot_rows, out_proj.T, preferred_element_type=jnp.float32).reshape(SEQ_DEV, LENGTH, INNER)
        grads_middle = middle_back(d_mixed)
        d_proj_low = grads_middle[0].astype(jnp.bfloat16).reshape(rows_block, PROJ)
        grad_in = jnp.dot(normed.T, d_proj_low, preferred_element_type=jnp.float32)
        d_normed = jnp.dot(d_proj_low, in_proj.T, preferred_element_type=jnp.float32).reshape(SEQ_DEV, LENGTH, D)
        grad_pre = lax.optimization_barrier(jnp.sum((d_normed * tokens_wide * inverse).reshape(rows_block, D), axis=0))
        d_scaled = d_normed * pre_wide
        d_tokens = cot_block.astype(jnp.float32) + inverse * d_scaled - tokens_wide * (inverse * inverse * inverse) * lax.optimization_barrier(jnp.mean(d_scaled * tokens_wide, axis=-1, keepdims=True))
        totals = (totals[0] + grad_in, totals[1] + grad_out, totals[2] + grad_pre) + tuple((total + grad for total, grad in zip(totals[3:], grads_middle[1:])))
        return (totals, (block_out, d_tokens))
    start = (jnp.zeros((D, PROJ), jnp.float32), jnp.zeros((INNER, D), jnp.float32), jnp.zeros((D,), jnp.float32)) + tuple((jnp.zeros(piece.shape, jnp.float32) for piece in small_params))
    totals, outputs = lax.scan(one_block, start, (token_blocks, cot_blocks))
    block_out = outputs[0].reshape(SEQS, LENGTH, D)
    grad_tokens = outputs[1].reshape(SEQS, LENGTH, D)
    return (block_out, grad_tokens, totals[0], totals[1], totals[2], totals[3], totals[4], totals[5], totals[6], totals[7], totals[8])
```

```python
import jax
import jax.numpy as jnp
from jax import lax
from jax.sharding import PartitionSpec as P

D = 1536
H = 48
P_SIZE = 64
NSTATE = 128
CONVK = 4
INNER = 3072
XBC = 3328
PROJ = 6448


epsilon = 1e-05
highest = lax.Precision.HIGHEST


def passed_along(block, axis, distance):
    devices = range(lax.axis_size(axis))
    route = [(i - distance, i) for i in devices if i - distance in devices]
    return lax.ppermute(block, axis, route)


def entering(value, axis, join, neutral, backward):
    count, mine = (lax.axis_size(axis), lax.axis_index(axis))
    pieces = jax.tree.map(lambda part: lax.all_gather(part, axis), value)
    if backward:
        pieces = jax.tree.map(lambda part: part[::-1], pieces)
        mine = count - 1 - mine
    total = jax.tree.map(
        lambda part, zero: jnp.full_like(part, 0) + jnp.asarray(zero, part.dtype), value, neutral
    )

    def turn(position, total):
        longer = join(total, jax.tree.map(lambda part: part[position], pieces))
        return jax.tree.map(lambda new, old: jnp.where(position < mine, new, old), longer, total)

    return lax.fori_loop(0, count - 1, turn, total)


def convolve(extended, conv_weight, conv_bias, seq_length):
    total = conv_bias
    for offset in range(CONVK):
        total = total + conv_weight[offset] * extended[:, offset : offset + seq_length]
    return total


def prepare(projected, halo_rows, conv_weight, conv_bias, dt_bias, a_log):
    seq_count, seq_length = (projected.shape[0], projected.shape[1])
    gate_z = projected[..., :INNER]
    extended = jnp.concatenate([halo_rows, projected[..., INNER : INNER + XBC]], axis=1)
    activated = jax.nn.silu(convolve(extended, conv_weight, conv_bias, seq_length))
    values = activated[..., :INNER].reshape(seq_count, seq_length, H, P_SIZE)
    b_state = activated[..., INNER : INNER + NSTATE]
    c_state = activated[..., INNER + NSTATE :]
    step_size = jax.nn.softplus(projected[..., INNER + XBC :] + dt_bias)
    log_decay = -step_size * jnp.exp(a_log)
    return (values, b_state, c_state, step_size, log_decay, gate_z)


def span_local(values, b_state, c_state, step_size, log_decay):
    seq_length = values.shape[1]
    cumulative = jnp.cumsum(log_decay, axis=1)
    inner_bc = jnp.einsum("stn,sun->stu", c_state, b_state, precision=highest)
    lower = jnp.arange(seq_length)[:, None] >= jnp.arange(seq_length)[None, :]
    differ = cumulative[:, :, None, :] - cumulative[:, None, :, :]
    kernel = (
        jnp.exp(jnp.where(lower[None, :, :, None], differ, -10000.0))
        * inner_bc[..., None]
        * step_size[:, None, :, :]
    )
    y_intra = jnp.einsum("stuh,suhp->sthp", kernel, values, precision=highest)
    decays = jnp.exp(cumulative)
    a_total = decays[:, -1, :]
    tail_weight = jnp.exp(cumulative[:, -1:, :] - cumulative) * step_size
    h_local = jnp.einsum("suh,suhp,sun->shpn", tail_weight, values, b_state, precision=highest)
    return (y_intra, decays, a_total, h_local)


def finish(y_intra, decays, c_state, h_enter, values, gate_z, d_skip, norm_gain):
    seq_count, seq_length = (values.shape[0], values.shape[1])
    y_inter = decays[..., None] * jnp.einsum("stn,shpn->sthp", c_state, h_enter, precision=highest)
    y_core = (y_intra + y_inter + d_skip[:, None] * values).reshape(seq_count, seq_length, INNER)
    gated = y_core * jax.nn.silu(gate_z)
    inverse = lax.rsqrt(jnp.mean(gated * gated, axis=-1, keepdims=True) + epsilon)
    return gated * inverse * norm_gain


def compose(earlier, later):
    return (earlier[0] * later[0], later[0][:, :, None, None] * earlier[1] + later[1])


def body(
    tokens,
    in_proj,
    out_proj,
    pre_gain,
    conv_weight,
    conv_bias,
    dt_bias,
    a_log,
    d_skip,
    norm_gain,
    cotangent,
):
    gathered = (
        lax.all_gather(in_proj, "shard", axis=0, tiled=True),
        lax.all_gather(out_proj, "shard", axis=0, tiled=True),
        lax.all_gather(pre_gain, "shard", axis=0, tiled=True),
        lax.all_gather(conv_weight, "shard", axis=1, tiled=True),
        lax.all_gather(conv_bias, "shard", axis=0, tiled=True),
        lax.all_gather(dt_bias, "shard", axis=0, tiled=True),
        lax.all_gather(a_log, "shard", axis=0, tiled=True),
        lax.all_gather(d_skip, "shard", axis=0, tiled=True),
        lax.all_gather(norm_gain, "shard", axis=0, tiled=True),
    )
    in_whole, out_whole = (gathered[0], gathered[1])
    small_params = tuple((piece.astype(jnp.float32) for piece in gathered[2:]))
    pre_whole = small_params[0]
    seq_count, seq_length = (tokens.shape[0], tokens.shape[1])
    rows_total = seq_count * seq_length
    tokens_wide = tokens.astype(jnp.float32)
    inverse = lax.rsqrt(jnp.mean(tokens_wide * tokens_wide, axis=-1, keepdims=True) + epsilon)
    normed = (tokens_wide * inverse * pre_whole).astype(jnp.bfloat16).reshape(rows_total, D)
    projected = jnp.dot(normed, in_whole, preferred_element_type=jnp.float32).reshape(
        seq_count, seq_length, PROJ
    )
    halo_rows = passed_along(
        projected[:, seq_length - (CONVK - 1) :, INNER : INNER + XBC], "seq", 1
    )
    prepared, prepare_back = jax.vjp(prepare, projected, halo_rows, *small_params[1:5])
    values, b_state, c_state, step_size, log_decay, gate_z = prepared
    span_out, span_back = jax.vjp(span_local, values, b_state, c_state, step_size, log_decay)
    y_intra, decays, a_total, h_local = span_out
    identity = (jnp.ones_like(a_total), jnp.zeros_like(h_local))
    h_enter = entering((a_total, h_local), "seq", compose, identity, False)[1]
    mixed, finish_back = jax.vjp(
        finish, y_intra, decays, c_state, h_enter, values, gate_z, small_params[5], small_params[6]
    )
    mixed_low = mixed.astype(jnp.bfloat16).reshape(rows_total, INNER)
    branch = jnp.dot(mixed_low, out_whole, preferred_element_type=jnp.float32)
    block_out = tokens_wide + branch.reshape(seq_count, seq_length, D)
    in_again, out_again = (
        lax.all_gather(in_proj, "shard", axis=0, tiled=True),
        lax.all_gather(out_proj, "shard", axis=0, tiled=True),
    )
    cot_rows = cotangent.reshape(rows_total, D)
    grad_out = jnp.dot(mixed_low.T, cot_rows, preferred_element_type=jnp.float32)
    d_mixed = jnp.dot(cot_rows, out_again.T, preferred_element_type=jnp.float32).reshape(
        seq_count, seq_length, INNER
    )
    d_intra, d_decays, d_cstate, d_enter, d_values, d_gate, grad_skip, grad_norm = finish_back(
        d_mixed
    )
    d_exit = entering((a_total, d_enter), "seq", compose, identity, True)[1]
    d_total = jnp.sum(d_exit * h_enter, axis=(2, 3))
    d_values_scan, d_bstate, d_cstate_scan, d_step, d_log = span_back(
        (d_intra, d_decays, d_total, d_exit)
    )
    d_projected, d_halo, grad_conv_weight, grad_conv_bias, grad_dt_bias, grad_a_log = prepare_back(
        (d_values + d_values_scan, d_bstate, d_cstate + d_cstate_scan, d_step, d_log, d_gate)
    )
    returned = passed_along(d_halo, "seq", -1)
    d_projected = d_projected.at[:, seq_length - (CONVK - 1) :, INNER : INNER + XBC].add(returned)
    d_proj_low = d_projected.astype(jnp.bfloat16).reshape(rows_total, PROJ)
    grad_in = jnp.dot(normed.T, d_proj_low, preferred_element_type=jnp.float32)
    d_normed = jnp.dot(d_proj_low, in_again.T, preferred_element_type=jnp.float32).reshape(
        seq_count, seq_length, D
    )
    grad_pre = jnp.sum((d_normed * tokens_wide * inverse).reshape(rows_total, D), axis=0)
    d_scaled = d_normed * pre_whole
    d_tokens = (
        cotangent.astype(jnp.float32)
        + inverse * d_scaled
        - tokens_wide
        * (inverse * inverse * inverse)
        * jnp.mean(d_scaled * tokens_wide, axis=-1, keepdims=True)
    )
    owned = (
        lax.psum_scatter(grad_in, "shard", scatter_dimension=0, tiled=True),
        lax.psum_scatter(grad_out, "shard", scatter_dimension=0, tiled=True),
        lax.psum_scatter(grad_pre, "shard", scatter_dimension=0, tiled=True),
        lax.psum_scatter(grad_conv_weight, "shard", scatter_dimension=1, tiled=True),
        lax.psum_scatter(grad_conv_bias, "shard", scatter_dimension=0, tiled=True),
        lax.psum_scatter(grad_dt_bias, "shard", scatter_dimension=0, tiled=True),
        lax.psum_scatter(grad_a_log, "shard", scatter_dimension=0, tiled=True),
        lax.psum_scatter(grad_skip, "shard", scatter_dimension=0, tiled=True),
        lax.psum_scatter(grad_norm, "shard", scatter_dimension=0, tiled=True),
    )
    summed = lax.psum(
        (owned[0], owned[1], owned[2], owned[3], owned[4], owned[5], owned[6], owned[7], owned[8]),
        ("seq", "replica"),
    )
    return (
        block_out,
        d_tokens,
        summed[0],
        summed[1],
        summed[2],
        summed[3],
        summed[4],
        summed[5],
        summed[6],
        summed[7],
        summed[8],
    )

f32, bf16 = jnp.float32, jnp.bfloat16


def chunk_step(state, piece):
    values, b_state, c_state, step_size, log_decay = piece
    y_intra, decays, a_total, h_local = span_local(values, b_state, c_state, step_size, log_decay)
    y_inter = decays[..., None] * jnp.einsum("stn,shpn->sthp", c_state, state, precision=highest)
    return a_total[:, :, None, None] * state + h_local, y_intra + y_inter


def core(xv, bc, dt_raw, conv_v, conv_bc, bias_v, bias_bc, dt_bias, a_log, d_skip):
    seqs, length = xv.shape[:2]
    heads = dt_raw.shape[-1]

    def act(raw, weight, bias):
        extended = jnp.pad(raw, ((0, 0), (CONVK - 1, 0), (0, 0)))
        return jax.nn.silu(convolve(extended, weight, bias, length))

    values = act(xv, conv_v, bias_v).reshape(seqs, length, heads, P_SIZE)
    state = act(bc, conv_bc, bias_bc)
    step_size = jax.nn.softplus(dt_raw + dt_bias)
    log_decay = -step_size * jnp.exp(a_log)
    span = min(256, length)
    pieces = tuple(
        jnp.moveaxis(p.reshape((seqs, length // span, span) + p.shape[2:]), 1, 0)
        for p in (values, state[..., :NSTATE], state[..., NSTATE:], step_size, log_decay)
    )
    start = jnp.zeros((seqs, heads, P_SIZE, NSTATE), f32)
    _, y = lax.scan(chunk_step, start, pieces, unroll=True)
    y = jnp.moveaxis(y, 0, 1).reshape(seqs, length, heads, P_SIZE)
    return (y + d_skip[:, None] * values).reshape(seqs, length, heads * P_SIZE)


TP = ("shard", "seq")


def split_body(
    tokens,
    in_proj,
    out_proj,
    pre_gain,
    conv_weight,
    conv_bias,
    dt_bias,
    a_log,
    d_skip,
    norm_gain,
    cotangent,
):
    n_shard, n_seq, n_rep = (lax.axis_size(a) for a in ("shard", "seq", "replica"))
    x, s = lax.axis_index("shard"), lax.axis_index("seq")
    ranks = n_shard * n_seq
    me = x * n_seq + s
    heads = H // ranks
    wide = INNER // ranks
    slim = 2 * NSTATE // ranks
    tok = tokens.reshape(-1, D)
    own_rows = tok.shape[0]
    seqs, length = n_shard, n_seq * own_rows
    rows = seqs * length
    kown = in_proj.shape[0]

    tok_all = lax.all_gather(tok, TP, axis=0, tiled=True)
    cot_all = lax.all_gather(cotangent.reshape(-1, D), TP, axis=0, tiled=True)

    def columns(rank):
        cut = lambda at, n: lax.dynamic_slice_in_dim(in_proj, at, n, 1)
        return jnp.concatenate(
            [
                cut(rank * wide, wide),
                cut(INNER + rank * wide, wide),
                in_proj[:, 2 * INNER : INNER + XBC],
                cut(INNER + XBC + rank * heads, heads),
            ],
            axis=1,
        )

    blocks = []
    for hop in range(n_shard):
        to = (x + hop) % n_shard
        piece = columns(to * n_seq + s)
        if hop:
            piece = lax.ppermute(piece, "shard", [(i, (i + hop) % n_shard) for i in range(n_shard)])
        blocks.append(piece)
    stack = jnp.stack(blocks)
    order = (x - jnp.arange(n_shard)) % n_shard
    w_own = stack[order].reshape(n_shard * kown, -1)
    small = jnp.concatenate(
        [
            p.reshape(-1)
            for p in (pre_gain, conv_weight, conv_bias, dt_bias, a_log, d_skip, norm_gain)
        ]
    )
    small = lax.all_gather(small, "shard", axis=0).astype(f32)
    sizes = (pre_gain.size, conv_weight.size, conv_bias.size, dt_bias.size, a_log.size, d_skip.size)
    at = [0]
    for n in sizes:
        at.append(at[-1] + n)
    pre_whole = small[:, at[0] : at[1]].reshape(-1)
    cw = small[:, at[1] : at[2]].reshape(n_shard, CONVK, -1)
    cw = jnp.moveaxis(cw, 0, 1).reshape(CONVK, XBC)
    cb = small[:, at[2] : at[3]].reshape(-1)
    own = lambda full, n: lax.dynamic_slice_in_dim(full.reshape(-1), me * n, n, 0)
    dtb = own(small[:, at[3] : at[4]], heads)
    alog = own(small[:, at[4] : at[5]], heads)
    skip = own(small[:, at[5] : at[6]], heads)
    gain = own(small[:, at[6] :], wide)
    conv_v = lax.dynamic_slice_in_dim(cw, me * wide, wide, 1)
    bias_v = lax.dynamic_slice_in_dim(cb, me * wide, wide, 0)
    conv_bc, bias_bc = cw[:, INNER:], cb[INNER:]
    out_own = lax.dynamic_slice_in_dim(out_proj, s * wide, wide, 0)

    wide_all = tok_all.astype(f32)
    inverse_all = lax.rsqrt(jnp.mean(wide_all * wide_all, axis=-1, keepdims=True) + epsilon)
    normed = (wide_all * inverse_all * pre_whole).astype(bf16)
    projected = jnp.dot(normed, w_own, preferred_element_type=f32).reshape(seqs, length, -1)
    gate = projected[..., :wide]
    xv = projected[..., wide : 2 * wide]
    bc = projected[..., 2 * wide : 2 * wide + 2 * NSTATE]
    dt_raw = projected[..., 2 * wide + 2 * NSTATE :]
    y_core, core_back = jax.vjp(
        core, xv, bc, dt_raw, conv_v, conv_bc, bias_v, bias_bc, dtb, alog, skip
    )
    sig = jax.nn.sigmoid(gate)
    silu = gate * sig
    gated = y_core * silu
    total = lax.psum(jnp.sum(gated * gated, axis=-1), TP)
    inv = lax.rsqrt(total / INNER + epsilon)[..., None]
    mixed = (gated * inv * gain).astype(bf16).reshape(rows, wide)
    branch = jnp.dot(mixed, out_own, preferred_element_type=f32).astype(bf16)
    branch = lax.psum_scatter(branch, TP, scatter_dimension=0, tiled=True)
    tok_wide = tok.astype(f32)
    block_out = tok_wide + branch.astype(f32)

    g_out = jnp.dot(mixed.T, cot_all, preferred_element_type=f32).astype(bf16)
    d_mixed = jnp.dot(cot_all, out_own.T, preferred_element_type=f32).reshape(seqs, length, wide)
    grad_gain = jnp.sum(d_mixed * gated * inv, axis=(0, 1))
    u = d_mixed * gain
    dot = lax.psum(jnp.sum(u * gated, axis=-1), TP)[..., None]
    d_gated = inv * u - gated * (inv * inv * inv) * (dot / INNER)
    d_y = d_gated * silu
    d_gate = d_gated * y_core * (sig * (1.0 + gate * (1.0 - sig)))
    d_xv, d_bc, d_dt, g_cv, g_cbc, g_bv, g_bbc, g_dtb, g_alog, g_skip = core_back(d_y)
    d_bc = lax.psum_scatter(d_bc.reshape(rows, -1), TP, scatter_dimension=1, tiled=True)
    d_own = jnp.concatenate(
        [
            d_gate.reshape(rows, wide).astype(bf16),
            d_xv.reshape(rows, wide).astype(bf16),
            d_bc.astype(bf16),
            d_dt.reshape(rows, heads).astype(bf16),
        ],
        axis=1,
    )
    w_back = jnp.concatenate(
        [
            w_own[:, : 2 * wide],
            lax.dynamic_slice_in_dim(w_own, 2 * wide + me * slim, slim, 1),
            w_own[:, 2 * wide + 2 * NSTATE :],
        ],
        axis=1,
    )
    d_normed = jnp.dot(d_own, w_back.T, preferred_element_type=f32).astype(bf16)
    d_normed = lax.psum_scatter(d_normed, TP, scatter_dimension=0, tiled=True).astype(f32)
    g_in = jnp.dot(normed.T, d_own, preferred_element_type=f32).astype(bf16)

    inverse = lax.rsqrt(jnp.mean(tok_wide * tok_wide, axis=-1, keepdims=True) + epsilon)
    grad_pre = jnp.sum(d_normed * tok_wide * inverse, axis=0)
    d_scaled = d_normed * pre_whole
    grad_tokens = (
        cotangent.reshape(-1, D).astype(f32)
        + inverse * d_scaled
        - tok_wide
        * (inverse * inverse * inverse)
        * jnp.mean(d_scaled * tok_wide, axis=-1, keepdims=True)
    )

    every = ("seq", "shard", "replica")
    place = lambda part, n, total_size: lax.dynamic_update_slice_in_dim(
        jnp.zeros(part.shape[:-1] + (total_size,), f32), part, n, part.ndim - 1
    )
    grad_cw = jnp.concatenate([place(g_cv, me * wide, INNER), g_cbc], axis=1)
    grad_cb = jnp.concatenate([place(g_bv, me * wide, INNER), g_bbc])
    smalls = lax.psum(
        (
            grad_pre,
            grad_cw,
            grad_cb,
            place(g_dtb, me * heads, H),
            place(g_alog, me * heads, H),
            place(g_skip, me * heads, H),
            place(grad_gain, me * wide, INNER),
        ),
        every,
    )
    mine = lambda full: lax.dynamic_slice_in_dim(
        full, x * (full.shape[-1] // n_shard), full.shape[-1] // n_shard, full.ndim - 1
    )
    smalls = [mine(v) for v in smalls]

    g_out = lax.psum_scatter(g_out, "replica", scatter_dimension=0, tiled=True)
    g_out = lax.all_gather(g_out, ("seq", "replica"), axis=0, tiled=True).astype(f32)
    g_in = g_in.reshape(n_shard, kown, -1)
    g_in = lax.psum_scatter(g_in, "replica", scatter_dimension=1, tiled=True)
    parts = []
    for hop in range(n_shard):
        piece = g_in[(x + hop) % n_shard]
        if hop:
            piece = lax.ppermute(piece, "shard", [(i, (i + hop) % n_shard) for i in range(n_shard)])
        parts.append(piece)
    g_in = jnp.stack(parts)[order]
    g_in = lax.all_gather(g_in, ("seq", "replica"))
    g_in = g_in.reshape((n_seq, n_rep) + g_in.shape[1:])
    g_in = jnp.transpose(g_in, (1, 3, 2, 0, 4)).reshape(kown, ranks, -1)
    cutat = (0, wide, 2 * wide, 2 * wide + slim, 2 * wide + slim + heads)
    g_in = jnp.concatenate(
        [g_in[:, :, a:b].reshape(kown, -1) for a, b in zip(cutat, cutat[1:])], axis=1
    ).astype(f32)
    return (
        block_out.reshape(tokens.shape),
        grad_tokens.reshape(tokens.shape),
        g_in,
        g_out,
        *smalls,
    )


def solution(mesh):
    in_specs = (
        P(("shard", "replica"), "seq", None),
        P("shard", None),
        P("shard", None),
        P("shard"),
        P(None, "shard"),
        P("shard"),
        P("shard"),
        P("shard"),
        P("shard"),
        P("shard"),
        P(("shard", "replica"), "seq", None),
    )
    out_specs = (
        P(("shard", "replica"), "seq", None),
        P(("shard", "replica"), "seq", None),
        P("shard", None),
        P("shard", None),
        P("shard"),
        P(None, "shard"),
        P("shard"),
        P("shard"),
        P("shard"),
        P("shard"),
        P("shard"),
    )
    ranks = mesh.shape["shard"] * mesh.shape["seq"]
    chosen = split_body if H % ranks == 0 and (INNER // ranks) % 128 == 0 else body
    return jax.shard_map(chosen, mesh=mesh, in_specs=in_specs, out_specs=out_specs, check_vma=False)
```
